128 devices in a mesh: dp: 16 (over y, x), row: 2 (over core), col: 4 (over z).
Axes of the slice: x: 4, y: 4, z: 4, core: 2. Of those that a mesh axis runs over, the one named last changes fastest.
Arguments:
- tokens: bfloat16 [15360, 4096], P(('dp', 'col'), 'row'), may hold values from -6 to 6
- hidden_cot: bfloat16 [15360, 14336], P(('dp', 'row'), 'col'), may hold values from -0.048339844 to 0.048339844
- gate_pre: bfloat16 [15360, 14336], P(('dp', 'row'), 'col'), may hold values from -10 to 10
- up_pre: bfloat16 [15360, 14336], P(('dp', 'row'), 'col'), may hold values from -6 to 6
Outputs:
- grad_gate: bfloat16 [2, 2048, 14336], P('row', 'dp', 'col')
The draws below stay inside these ranges and needn't reach their ends.
All inputs are finite; a program needn't handle non-finite values.
Results may differ from the reference program's by a relative error of at most 0.014.
Values may be sent and summed in bfloat16 or wider, within the bound.
A program may use at most 128 MiB of HBM per device.

```python
import jax
import jax.numpy as jnp
from jax import lax

D = 4096
FF = 14336
GROUP_TOK = 960
TOKENS = 15360
N_DP = 16
N_ROW = 2


def level_of(own_key, shape, split, least, high):
    def one(dim, parts):
        heights = jax.random.uniform(jax.random.fold_in(jax.random.fold_in(own_key, 6), dim), (parts,), jnp.float32, least / len(split), high / len(split))
        return jnp.repeat(jnp.exp(heights), shape[dim] // parts).reshape((-1,) + (1,) * (len(shape) - dim - 1))

    gain = one(*split[0])
    for cut in split[1:]:
        gain = gain * one(*cut)
    return gain


def scatter_about(own_key, dims, deviation, most, shards=(), held_as=jnp.bfloat16):
    drawn = deviation * jax.random.normal(own_key, dims, jnp.float32)
    if shards:
        drawn = drawn * level_of(own_key, dims, shards, -0.22, 0.18)
    return jnp.clip(drawn, -most, most).astype(held_as)


def setup_inputs(seed: int = 0) -> dict:
    seeds = jax.random.split(jax.random.key(seed), 5)
    return {
        "tokens": scatter_about(seeds[0], (TOKENS, D), 1.0, 6.0, ((0, 64), (1, 2))),
        "hidden_cot": scatter_about(seeds[1], (TOKENS, FF), (TOKENS ** -0.5), 0.048339844, ((0, 32), (1, 4))),
        "gate_pre": scatter_about(seeds[2], (TOKENS, FF), 2.0, 10.0, ((0, 32), (1, 4))),
        "up_pre": scatter_about(seeds[3], (TOKENS, FF), 1.0, 6.0, ((0, 32), (1, 4))),
    }


def reference(tokens, hidden_cot, gate_pre, up_pre):
    gate_val = gate_pre.astype(jnp.float32)
    up_val = up_pre.astype(jnp.float32)
    cot_val = hidden_cot.astype(jnp.float32)
    sigma = jax.nn.sigmoid(gate_val)
    gate_grad = (cot_val * up_val * sigma * (1.0 + gate_val * (1.0 - sigma))).astype(jnp.bfloat16)
    tok_groups = tokens.reshape(N_DP, GROUP_TOK, D)
    grad_groups = gate_grad.reshape(N_DP, GROUP_TOK, FF)

    def one_group(total, pair):
        part = jnp.dot(pair[0].T, pair[1], preferred_element_type=jnp.float32).astype(jnp.bfloat16)
        return total + part.astype(jnp.float32), None

    summed, _ = lax.scan(one_group, jnp.zeros((D, FF), jnp.float32), (tok_groups, grad_groups))
    return summed.astype(jnp.bfloat16).reshape(N_ROW, D // N_ROW, FF)
```

```python
import jax
import jax.numpy as jnp
from jax import lax
from jax.experimental import pallas as pl
from jax.experimental.pallas import tpu as pltpu
from jax.sharding import PartitionSpec as P

MESH = pl.DeviceIdType.MESH
SIDE = 4
CORES = 2
DEPTH = 4
ORDER = (
    (2, 2), (2, 1), (2, 3), (1, 2), (3, 2), (2, 0), (0, 2), (1, 1),
    (1, 3), (3, 1), (3, 3), (1, 0), (3, 0), (0, 1), (0, 3), (0, 0),
)
STEP = {2: 0, 1: 1, 3: 2, 0: 3}
FLOWS = 4
FAR, JOINED, DIRECT = 0, 1, 2


def kernel(
    tok_in, cot_in, gate_in, up_in, out,
    tok, tok_t, cot, gate, up, grad, part, inbox, inbox2,
    local_sem, gate_sem, out_sem,
    tok_send, tok_recv, grad_send, grad_recv,
    send1, recv1, send2, recv2,
):
    share, own_rows = tok_in.shape[0], cot_in.shape[0]
    lanes = tok.shape[2]
    width = grad.shape[1] // FLOWS
    dp = lax.axis_index("dp")
    core = lax.axis_index("row")
    z = lax.axis_index("col")
    y, x = lax.div(dp, SIDE), lax.rem(dp, SIDE)

    def shift(index, by):
        return lax.rem(index + by, SIDE)

    def along(axis, by):
        if axis == "x":
            return {"dp": y * SIDE + shift(x, by % SIDE)}
        return {"dp": shift(y, by % SIDE) * SIDE + x}

    z_up, z_down = {"col": shift(z, 1)}, {"col": shift(z, DEPTH - 1)}
    partner = {"row": 1 - core}

    def remote(src, dst, ss, rs, device):
        return pltpu.make_async_remote_copy(
            src_ref=src, dst_ref=dst, send_sem=ss, recv_sem=rs,
            device_id=device, device_id_type=MESH,
        )

    def tok_rows(k, owner):
        rows = pl.ds(pl.multiple_of(owner * share, 16), share)
        return tok.at[k, rows, :]

    def load_tokens(k):
        dy, dx = ORDER[k]
        owner = shift(y, dy) * SIDE + shift(x, dx)
        columns = pl.ds(pl.multiple_of(owner * lanes, lanes), lanes)
        return pltpu.make_async_copy(
            tok_in.at[:, columns], tok_rows(k, z), local_sem.at[k]
        )

    def columns_of(c):
        return slice(c * width, (c + 1) * width)

    def load_gates(c):
        return [
            pltpu.make_async_copy(
                src.at[:, columns_of(c)], dst.at[:, columns_of(c)], gate_sem.at[i, c]
            )
            for i, (src, dst) in enumerate(((cot_in, cot), (gate_in, gate), (up_in, up)))
        ]

    for k in range(4):
        load_tokens(k).start()
    for c in range(FLOWS):
        for copy in load_gates(c):
            copy.start()
    for k in range(4, len(ORDER)):
        load_tokens(k).start()

    neighbours = [partner, z_up, z_down] + [
        along(axis, by) for axis in "xy" for by in (1, -1)
    ]
    barrier = pltpu.get_barrier_semaphore()
    for device in neighbours:
        pl.semaphore_signal(barrier, inc=1, device_id=device, device_id_type=MESH)
    pl.semaphore_wait(barrier, len(neighbours))

    def tok_copy(k, i):
        if i < 2:
            rows, to = tok_rows(k, z), (z_up, z_down)[i]
        elif k % 2 == 0:
            rows, to = tok_rows(k, shift(z, DEPTH - 1)), z_up
        else:
            rows, to = tok_rows(k, shift(z, 1)), z_down
        return remote(rows, rows, tok_send.at[k, i], tok_recv.at[k, i], to)

    def arrival(k, i):
        source = shift(z, (DEPTH - 1, 1, 2)[i])
        rows = tok_rows(k, source)
        return remote(rows, rows, tok_send.at[k, i], tok_recv.at[k, i], z_up)

    def give_tokens(k):
        if k < len(ORDER):
            load_tokens(k).wait()
            tok_copy(k, 0).start()
            tok_copy(k, 1).start()

    def pass_tokens(k):
        if k < len(ORDER):
            arrival(k, k % 2).wait_recv()
            tok_copy(k, 2).start()

    def await_tokens(k):
        arrival(k, 1 - k % 2).wait_recv()
        arrival(k, 2).wait_recv()

    own_offset = pl.multiple_of(core * own_rows, 16)

    def grad_rows(c, offset):
        return grad.at[pl.ds(pl.multiple_of(offset, 16), own_rows), columns_of(c)]

    def grad_copy(c):
        mine = grad_rows(c, own_offset)
        return remote(mine, mine, grad_send.at[c], grad_recv.at[c], partner)

    def grad_arrival(c):
        theirs = grad_rows(c, (1 - core) * own_rows)
        return remote(theirs, theirs, grad_send.at[c], grad_recv.at[c], partner)

    def make_grad(c):
        for copy in load_gates(c):
            copy.wait()

        def rows_of(i, carry):
            rows = pl.ds(pl.multiple_of(i * 16, 16), 16)
            g = gate[rows, columns_of(c)].astype(jnp.float32)
            u = up[rows, columns_of(c)].astype(jnp.float32)
            h = cot[rows, columns_of(c)].astype(jnp.float32)
            s = jax.nn.sigmoid(g)
            there = pl.ds(pl.multiple_of(own_offset + i * 16, 16), 16)
            grad[there, columns_of(c)] = (h * u * s * (1.0 + g * (1.0 - s))).astype(grad.dtype)
            return carry

        lax.fori_loop(0, own_rows // 16, rows_of, 0)
        grad_copy(c).start()

    def axes_of(q):
        return ("x", "y") if q < 2 else ("y", "x")

    def sign_of(q):
        return 1 if q % 2 == 0 else -1

    def block_of(q, first, second):
        offsets = (second % SIDE, first % SIDE) if q < 2 else (first % SIDE, second % SIDE)
        return ORDER.index(offsets)

    def unit(k, q):
        return part.at[k, :, columns_of(q)]

    def copy1(q, role, j, src=None):
        axis, sign = axes_of(q)[0], sign_of(q)
        box = inbox.at[q, role, j]
        device = along(axis, -sign if role == DIRECT else sign)
        return remote(
            box if src is None else src, box,
            send1.at[q, role, j], recv1.at[q, role, j], device,
        )

    def copy2(q, role, src=None):
        axis, sign = axes_of(q)[1], sign_of(q)
        box = inbox2.at[q, role]
        device = along(axis, -sign if role == DIRECT else sign)
        return remote(
            box if src is None else src, box,
            send2.at[q, role], recv2.at[q, role], device,
        )

    def add_into(dst, *terms):
        rows_all = dst.shape[0]

        def rows_of(i, carry):
            rows = pl.ds(pl.multiple_of(i * 16, 16), 16)
            total = dst[rows, :].astype(jnp.float32)
            for term in terms:
                total = total + term[rows, :].astype(jnp.float32)
            dst[rows, :] = total.astype(dst.dtype)
            return carry

        lax.fori_loop(0, rows_all // 16, rows_of, 0)

    def send_first(k, q):
        dy, dx = ORDER[k]
        first, second = (dx, dy) if q < 2 else (dy, dx)
        sign = sign_of(q)
        if first == 2:
            role = FAR
        elif first == -sign % SIDE:
            role = DIRECT
        else:
            return
        copy1(q, role, STEP[second], unit(k, q)).start()

    def join(q, second):
        j = STEP[second % SIDE]
        mine = unit(block_of(q, sign_of(q), second), q)
        copy1(q, FAR, j).wait_recv()
        add_into(mine, inbox.at[q, FAR, j])
        copy1(q, JOINED, j, mine).start()

    def settle(q, second, *more):
        j = STEP[second % SIDE]
        mine = unit(block_of(q, 0, second), q)
        copy1(q, JOINED, j).wait_recv()
        copy1(q, DIRECT, j).wait_recv()
        add_into(mine, inbox.at[q, JOINED, j], inbox.at[q, DIRECT, j], *more)
        return mine

    def far_second(q):
        copy2(q, FAR, settle(q, 2)).start()

    def direct_second(q):
        copy2(q, DIRECT, settle(q, -sign_of(q))).start()

    def join_second(q):
        copy2(q, FAR).wait_recv()
        mine = settle(q, sign_of(q), inbox2.at[q, FAR])
        copy2(q, JOINED, mine).start()

    def write(q):
        return pltpu.make_async_copy(
            unit(block_of(q, 0, 0), q), out.at[0, :, columns_of(q)], out_sem.at[q]
        )

    def finish(q):
        copy2(q, JOINED).wait_recv()
        copy2(q, DIRECT).wait_recv()
        settle(q, 0, inbox2.at[q, JOINED], inbox2.at[q, DIRECT])
        write(q).start()

    flows = range(FLOWS)

    def after(k):
        if k == 5:
            for q in flows:
                join(q, 2)
        elif k == 9:
            for q in flows:
                join(q, 1)
        elif k == 11:
            for q in flows:
                join(q, 3)
        elif k == 14:
            for q in flows:
                far_second(q)

    give_tokens(0)
    give_tokens(1)
    make_grad(0)
    make_grad(1)
    pass_tokens(0)
    give_tokens(2)
    make_grad(2)
    pass_tokens(1)
    give_tokens(3)
    make_grad(3)
    pass_tokens(2)
    give_tokens(4)

    half = 2 * width

    def block(b, carry):
        for k in range(len(ORDER)):

            @pl.when(b == k)
            def _(k=k):
                pass_tokens(k + 3)
                give_tokens(k + 5)
                await_tokens(k)
                if k == 0:
                    for c in flows:
                        grad_arrival(c).wait_recv()

        tok_t[...] = tok[b].T
        for pair in range(2):
            part[b, :, pair * half:(pair + 1) * half] = jnp.dot(
                tok_t[...], grad[:, pair * half:(pair + 1) * half],
                preferred_element_type=jnp.float32,
            ).astype(part.dtype)
            for k in range(len(ORDER)):

                @pl.when(b == k)
                def _(k=k, pair=pair):
                    send_first(k, 2 * pair)
                    send_first(k, 2 * pair + 1)
                    if pair == 1:
                        after(k)

        return carry

    lax.fori_loop(0, len(ORDER), block, 0)

    for q in flows:
        join(q, 0)
    for q in flows:
        direct_second(q)
    for q in flows:
        join_second(q)
    for q in flows:
        finish(q)

    for k in range(len(ORDER)):
        for i in range(3):
            tok_copy(k, i).wait_send()
    for c in flows:
        grad_copy(c).wait_send()
    for q in flows:
        for role in (FAR, JOINED, DIRECT):
            for j in range(SIDE):
                copy1(q, role, j).wait_send()
            copy2(q, role).wait_send()
    for q in flows:
        write(q).wait()


def on_device(tokens, hidden_cot, gate_pre, up_pre):
    share, model = tokens.shape
    own_rows, hidden = hidden_cot.shape
    lanes = model // len(ORDER)
    width = hidden // FLOWS
    dtype = tokens.dtype
    dma = pltpu.SemaphoreType.DMA
    any_space = pl.BlockSpec(memory_space=pl.ANY)
    return pl.pallas_call(
        kernel,
        out_shape=jax.ShapeDtypeStruct((1, lanes, hidden), dtype),
        in_specs=[any_space] * 4,
        out_specs=any_space,
        scratch_shapes=[
            pltpu.VMEM((len(ORDER), DEPTH * share, lanes), dtype),
            pltpu.VMEM((lanes, DEPTH * share), dtype),
            pltpu.VMEM((own_rows, hidden), dtype),
            pltpu.VMEM((own_rows, hidden), dtype),
            pltpu.VMEM((own_rows, hidden), dtype),
            pltpu.VMEM((CORES * own_rows, hidden), dtype),
            pltpu.VMEM((len(ORDER), lanes, hidden), dtype),
            pltpu.VMEM((FLOWS, 3, SIDE, lanes, width), dtype),
            pltpu.VMEM((FLOWS, 3, lanes, width), dtype),
            dma((len(ORDER),)),
            dma((3, FLOWS)),
            dma((FLOWS,)),
            dma((len(ORDER), 3)),
            dma((len(ORDER), 3)),
            dma((FLOWS,)),
            dma((FLOWS,)),
            dma((FLOWS, 3, SIDE)),
            dma((FLOWS, 3, SIDE)),
            dma((FLOWS, 3)),
            dma((FLOWS, 3)),
        ],
        compiler_params=pltpu.CompilerParams(
            collective_id=0, has_side_effects=True, vmem_limit_bytes=62 * 2**20
        ),
    )(tokens, hidden_cot, gate_pre, up_pre)


def solution(mesh):
    in_specs = (
        P(("dp", "col"), "row"),
        P(("dp", "row"), "col"),
        P(("dp", "row"), "col"),
        P(("dp", "row"), "col"),
    )
    out_specs = P("row", "dp", "col")
    return jax.shard_map(
        on_device, mesh=mesh, in_specs=in_specs, out_specs=out_specs, check_vma=False
    )
```

```python
import jax
import jax.numpy as jnp
from jax import lax
from jax.experimental import pallas as pl
from jax.experimental.pallas import tpu as pltpu
from jax.sharding import PartitionSpec as P

MESH = pl.DeviceIdType.MESH
SIDE = 4
CORES = 2
DEPTH = 4
ORDER = (
    (2, 2), (2, 1), (2, 3), (1, 2), (3, 2), (2, 0), (0, 2), (1, 1),
    (1, 3), (3, 1), (3, 3), (1, 0), (3, 0), (0, 1), (0, 3), (0, 0),
)
STEP = {2: 0, 1: 1, 3: 2, 0: 3}
FLOWS = 4
FAR, JOINED, DIRECT = 0, 1, 2
GROUPS = ((0, 1), (1, 2), (2, 4), (4, 8), (8, 16))


def kernel(
    tok_in, cot_in, gate_in, up_in, out,
    tok, tok_t, gates, grad, part, inbox, inbox2,
    local_sem, gate_sem, out_sem,
    tok_send, tok_recv, grad_send, grad_recv,
    send1, far1, near1, send2, far2, near2,
):
    share, own_rows = tok_in.shape[0], cot_in.shape[0]
    lanes = tok.shape[2]
    width = grad.shape[1] // FLOWS
    dp = lax.axis_index("dp")
    core = lax.axis_index("row")
    z = lax.axis_index("col")
    y, x = lax.div(dp, SIDE), lax.rem(dp, SIDE)

    def shift(index, by):
        return lax.rem(index + by, SIDE)

    def along(axis, by):
        if axis == "x":
            return {"dp": y * SIDE + shift(x, by % SIDE)}
        return {"dp": shift(y, by % SIDE) * SIDE + x}

    z_up, z_down = {"col": shift(z, 1)}, {"col": shift(z, DEPTH - 1)}
    z_across = {"col": shift(z, 2)}
    partner = {"row": 1 - core}

    def remote(src, dst, ss, rs, device):
        return pltpu.make_async_remote_copy(
            src_ref=src, dst_ref=dst, send_sem=ss, recv_sem=rs,
            device_id=device, device_id_type=MESH,
        )

    def tok_rows(k, owner):
        rows = pl.ds(pl.multiple_of(owner * share, 16), share)
        return tok.at[k, rows, :]

    def group_of(k):
        return next(i for i, (first, end) in enumerate(GROUPS) if first <= k < end)

    def load_tokens(k):
        dy, dx = ORDER[k]
        owner = shift(y, dy) * SIDE + shift(x, dx)
        columns = pl.ds(pl.multiple_of(owner * lanes, lanes), lanes)
        return pltpu.make_async_copy(
            tok_in.at[:, columns], tok_rows(k, z), local_sem.at[group_of(k)]
        )

    def columns_of(c):
        return slice(c * width, (c + 1) * width)

    def load_gates(c):
        for i, src in enumerate((cot_in, gate_in, up_in)):
            pltpu.make_async_copy(
                src.at[:, columns_of(c)], gates.at[i, :, columns_of(c)], gate_sem.at[c]
            ).start()

    def wait_for(ref, sem):
        pltpu.make_async_copy(ref, ref, sem).wait()

    for k in range(4):
        load_tokens(k).start()
    for c in range(FLOWS):
        load_gates(c)
    for k in range(4, len(ORDER)):
        load_tokens(k).start()

    neighbours = [partner, z_up, z_down, z_across] + [
        along(axis, by) for axis in "xy" for by in (1, -1)
    ]
    barrier = pltpu.get_barrier_semaphore()
    for device in neighbours:
        pl.semaphore_signal(barrier, inc=1, device_id=device, device_id_type=MESH)
    pl.semaphore_wait(barrier, len(neighbours))

    def tok_copy(k, i):
        if i < 2:
            rows, to = tok_rows(k, z), (z_up, z_down)[i]
        elif k == 0:
            rows, to = tok_rows(k, z), z_across
        elif k % 2 == 0:
            rows, to = tok_rows(k, shift(z, DEPTH - 1)), z_up
        else:
            rows, to = tok_rows(k, shift(z, 1)), z_down
        return remote(rows, rows, tok_send, tok_recv.at[k, 0 if i == k % 2 else 1], to)

    def give_tokens(k):
        if k < len(ORDER):
            first, end = GROUPS[group_of(k)]
            if k == first:
                rows = pl.ds(pl.multiple_of(z * share, 16), share)
                wait_for(tok.at[first:end, rows, :], local_sem.at[group_of(k)])
            tok_copy(k, 0).start()
            tok_copy(k, 1).start()
            if k == 0:
                tok_copy(k, 2).start()

    def pass_tokens(k):
        if k < len(ORDER):
            wait_for(tok_rows(k, shift(z, (DEPTH - 1, 1)[k % 2])), tok_recv.at[k, 0])
            tok_copy(k, 2).start()

    def await_tokens(k):
        if k == 0:
            wait_for(tok_rows(k, shift(z, DEPTH - 1)), tok_recv.at[k, 0])
        wait_for(tok.at[k, :2 * share, :], tok_recv.at[k, 1])

    own_offset = pl.multiple_of(core * own_rows, 16)

    def grad_rows(c, offset):
        return grad.at[pl.ds(pl.multiple_of(offset, 16), own_rows), columns_of(c)]

    def grad_copy(c):
        mine = grad_rows(c, own_offset)
        return remote(mine, mine, grad_send, grad_recv.at[c], partner)

    def await_grad(c):
        wait_for(grad_rows(c, (1 - core) * own_rows), grad_recv.at[c])

    def make_grad(c):
        wait_for(gates.at[:, :, columns_of(c)], gate_sem.at[c])

        def rows_of(n, carry):
            rows = pl.ds(pl.multiple_of(n * 16, 16), 16)
            h, g, u = (gates[i, rows, columns_of(c)].astype(jnp.float32) for i in range(3))
            s = jax.nn.sigmoid(g)
            there = pl.ds(pl.multiple_of(own_offset + n * 16, 16), 16)
            grad[there, columns_of(c)] = (h * u * s * (1.0 + g * (1.0 - s))).astype(grad.dtype)
            return carry

        lax.fori_loop(0, own_rows // 16, rows_of, 0)
        grad_copy(c).start()

    def axes_of(q):
        return ("x", "y") if q < 2 else ("y", "x")

    def sign_of(q):
        return 1 if q % 2 == 0 else -1

    def block_of(q, first, second):
        offsets = (second % SIDE, first % SIDE) if q < 2 else (first % SIDE, second % SIDE)
        return ORDER.index(offsets)

    def unit(k, q):
        return part.at[k, :, columns_of(q)]

    def send1_to(q, role, j, src):
        axis, sign = axes_of(q)[0], sign_of(q)
        arrived = far1.at[q, j] if role == FAR else near1.at[q, j]
        device = along(axis, -sign if role == DIRECT else sign)
        remote(src, inbox.at[q, role, j], send1, arrived, device).start()

    def send2_to(q, role, src):
        axis, sign = axes_of(q)[1], sign_of(q)
        arrived = far2.at[q] if role == FAR else near2.at[q]
        device = along(axis, -sign if role == DIRECT else sign)
        remote(src, inbox2.at[q, role], send2, arrived, device).start()

    def add_into(dst, *terms):
        rows_all = dst.shape[0]

        def rows_of(i, carry):
            rows = pl.ds(pl.multiple_of(i * 16, 16), 16)
            total = dst[rows, :].astype(jnp.float32)
            for term in terms:
                total = total + term[rows, :].astype(jnp.float32)
            dst[rows, :] = total.astype(dst.dtype)
            return carry

        lax.fori_loop(0, rows_all // 16, rows_of, 0)

    def send_first(k, q):
        dy, dx = ORDER[k]
        first, second = (dx, dy) if q < 2 else (dy, dx)
        sign = sign_of(q)
        if first == 2:
            role = FAR
        elif first == -sign % SIDE:
            role = DIRECT
        else:
            return
        send1_to(q, role, STEP[second], unit(k, q))

    def join(q, second):
        j = STEP[second % SIDE]
        mine = unit(block_of(q, sign_of(q), second), q)
        wait_for(inbox.at[q, FAR, j], far1.at[q, j])
        add_into(mine, inbox.at[q, FAR, j])
        send1_to(q, JOINED, j, mine)

    def settle(q, second, *more):
        j = STEP[second % SIDE]
        mine = unit(block_of(q, 0, second), q)
        wait_for(inbox.at[q, JOINED:, j], near1.at[q, j])
        add_into(mine, inbox.at[q, JOINED, j], inbox.at[q, DIRECT, j], *more)
        return mine

    def far_second(q):
        send2_to(q, FAR, settle(q, 2))

    def direct_second(q):
        send2_to(q, DIRECT, settle(q, -sign_of(q)))

    def join_second(q):
        wait_for(inbox2.at[q, FAR], far2.at[q])
        send2_to(q, JOINED, settle(q, sign_of(q), inbox2.at[q, FAR]))

    def write(q):
        mine = unit(block_of(q, 0, 0), q)
        pltpu.make_async_copy(mine, out.at[0, :, columns_of(q)], out_sem).start()

    def finish(q):
        wait_for(inbox2.at[q, JOINED:], near2.at[q])
        settle(q, 0, inbox2.at[q, JOINED], inbox2.at[q, DIRECT])
        write(q)

    flows = range(FLOWS)

    def after(k):
        if k == 5:
            for q in flows:
                join(q, 2)
        elif k == 9:
            for q in flows:
                join(q, 1)
        elif k == 11:
            for q in flows:
                join(q, 3)
        elif k == 14:
            for q in flows:
                far_second(q)

    def multiply(b, columns):
        part[b, :, columns] = jnp.dot(
            tok_t[...], grad[:, columns], preferred_element_type=jnp.float32
        ).astype(part.dtype)

    give_tokens(0)
    give_tokens(1)
    make_grad(0)
    give_tokens(2)
    make_grad(1)
    make_grad(2)
    give_tokens(3)
    make_grad(3)
    await_tokens(0)
    tok_t[...] = tok[0].T
    for q in flows:
        await_grad(q)
        multiply(0, columns_of(q))
        send_first(0, q)
        if q == 1:
            pass_tokens(1)
            give_tokens(4)
    pass_tokens(2)
    give_tokens(5)

    half = 2 * width

    def block(b, carry):
        for k in range(1, len(ORDER)):

            @pl.when(b == k)
            def _(k=k):
                pass_tokens(k + 2)
                give_tokens(k + 5)
                await_tokens(k)

        tok_t[...] = tok[b].T
        for pair in range(2):
            multiply(b, slice(pair * half, (pair + 1) * half))
            for k in range(1, len(ORDER)):

                @pl.when(b == k)
                def _(k=k, pair=pair):
                    send_first(k, 2 * pair)
                    send_first(k, 2 * pair + 1)
                    if pair == 1:
                        after(k)

        return carry

    lax.fori_loop(1, len(ORDER), block, 0)

    for q in flows:
        join(q, 0)
    for q in flows:
        direct_second(q)
    for q in flows:
        join_second(q)
    for q in flows:
        finish(q)

    wait_for(tok.at[:, :3 * share, :], tok_send)
    wait_for(gates.at[0], grad_send)
    wait_for(inbox, send1)
    wait_for(inbox2, send2)
    wait_for(part.at[0], out_sem)


def on_device(tokens, hidden_cot, gate_pre, up_pre):
    share, model = tokens.shape
    own_rows, hidden = hidden_cot.shape
    lanes = model // len(ORDER)
    width = hidden // FLOWS
    dtype = tokens.dtype
    dma = pltpu.SemaphoreType.DMA
    any_space = pl.BlockSpec(memory_space=pl.ANY)
    return pl.pallas_call(
        kernel,
        out_shape=jax.ShapeDtypeStruct((1, lanes, hidden), dtype),
        in_specs=[any_space] * 4,
        out_specs=any_space,
        scratch_shapes=[
            pltpu.VMEM((len(ORDER), DEPTH * share, lanes), dtype),
            pltpu.VMEM((lanes, DEPTH * share), dtype),
            pltpu.VMEM((3, own_rows, hidden), dtype),
            pltpu.VMEM((CORES * own_rows, hidden), dtype),
            pltpu.VMEM((len(ORDER), lanes, hidden), dtype),
            pltpu.VMEM((FLOWS, 3, SIDE, lanes, width), dtype),
            pltpu.VMEM((FLOWS, 3, lanes, width), dtype),
            dma((len(GROUPS),)),
            dma((FLOWS,)),
            dma,
            dma,
            dma((len(ORDER), 2)),
            dma,
            dma((FLOWS,)),
            dma,
            dma((FLOWS, SIDE)),
            dma((FLOWS, SIDE)),
            dma,
            dma((FLOWS,)),
            dma((FLOWS,)),
        ],
        compiler_params=pltpu.CompilerParams(
            collective_id=0, has_side_effects=True, vmem_limit_bytes=53 * 2**20
        ),
    )(tokens, hidden_cot, gate_pre, up_pre)


def solution(mesh):
    in_specs = (
        P(("dp", "col"), "row"),
        P(("dp", "row"), "col"),
        P(("dp", "row"), "col"),
        P(("dp", "row"), "col"),
    )
    out_specs = P("row", "dp", "col")
    return jax.shard_map(
        on_device, mesh=mesh, in_specs=in_specs, out_specs=out_specs, check_vma=False
    )
```
